32 devices in a mesh: row: 4 (over y, core), phi: 8 (over z, x).
Axes of the slice: x: 2, y: 2, z: 4, core: 2. Of those that a mesh axis runs over, the one named last changes fastest.
Arguments:
- hydro_vars: float32 [5, 128, 128, 256], P(None, 'row', 'phi'), may hold values from -6 to 6
- face_b: float32 [3, 128, 128, 256], P(None, 'row', 'phi'), may hold values from -6 to 6
- widths: int32 [16], replicated, may hold values from 2 to 128, as said below
- diffusion: float32 [5, 256], replicated, may hold values from 0.01 to 0.06
Outputs:
- conserved: float32 [8, 128, 128, 256], P(None, 'row', 'phi')
- faces_out: float32 [3, 128, 128, 256], P(None, 'row', 'phi')
The draws below stay inside these ranges and needn't reach their ends.
Inputs may be any that keep to these rules, and one draw needn't show every extreme that they name: `widths`: every width is a power of two that divides 128; the two cycles next to the poles (entries 0 and 15) use 128.
All inputs are finite; a program needn't handle non-finite values.
Results may differ from the reference program's by a relative error of at most 0.0001.
Values sent between devices are 32-bit elements; how exact they have to be, the bound alone decides.
No kernel may reach another device: no remote copies, remote signals or barrier semaphores. Data moves between devices by JAX's collectives and lax.ppermute only.
A program may use at most 64 MiB of HBM per device.

```python
import math
import jax
import jax.numpy as jnp
from jax import lax

NTH = 256
CYCLES = 8
NR = 128
PHI_CELLS = 128


def draw_widths(key, part):
    top = PHI_CELLS.bit_length() - 1
    powers = jax.random.randint(jax.random.fold_in(key, 7), (2 * CYCLES,), 1, top + 1)
    powers = powers.at[0].set(top).at[2 * CYCLES - 1].set(top)
    return jnp.power(2, powers).astype(jnp.int32)


def block_scale(rng, extent, pieces, low, high):
    loudness, own = 1.0, jax.random.fold_in(rng, 6)
    for position, blocks in pieces:
        draws = jnp.exp(jax.random.uniform(jax.random.fold_in(own, position), (blocks,), jnp.float32, low / len(pieces), high / len(pieces)))
        loudness = loudness * jnp.repeat(draws, extent[position] // blocks).reshape([-1 if axis == position else 1 for axis in range(len(extent))])
    return loudness


def centred(rng, extent, scale, limit, cuts=(), kind=jnp.bfloat16):
    values = jax.random.normal(rng, extent, jnp.float32) * scale
    if len(cuts) > 0:
        values = block_scale(rng, extent, cuts, -0.22, 0.18) * values
    return jnp.clip(values, min=-limit, max=limit).astype(kind)


def setup_inputs(seed: int = 0) -> dict:
    key_of = jax.random.split(jax.random.key(seed), 5)
    hydro_vars = centred(key_of[0], (5, NR, PHI_CELLS, NTH), 1.0, 6.0, ((1, 4), (2, 8)), jnp.float32)
    face_b = centred(key_of[1], (3, NR, PHI_CELLS, NTH), 1.0, 6.0, ((1, 4), (2, 8)), jnp.float32)
    widths = draw_widths(jax.random.fold_in(key_of[4], 71), 0)
    diffusion = jnp.clip(jnp.exp(jax.random.uniform(key_of[3], (5, NTH), jnp.float32, math.log(0.01), math.log(0.06))), 0.01, 0.06)
    return dict(hydro_vars=hydro_vars, face_b=face_b, widths=widths, diffusion=diffusion)


def stencil(padded, axis, count):
    parts = [lax.slice_in_dim(padded, offset, offset + count, axis=axis) for offset in range(5)]
    return (16.0 * (parts[1] + parts[3]) - (parts[0] + parts[4]) - 30.0 * parts[2]) / 12.0


def fourth(values, axis, wrapped):
    count = values.shape[axis]
    pads = [(0, 0)] * values.ndim
    pads[axis] = (2, 2)
    padded = jnp.pad(values, pads, mode="wrap") if wrapped else jnp.pad(values, pads)
    return stencil(padded, axis, count)


def block_means(cycles, axis, width):
    cells = cycles.shape[axis]
    result = cycles
    for power in range(1, cells.bit_length()):
        size = 2 ** power
        shape = cycles.shape[:axis] + (cells // size, size) + cycles.shape[axis + 1:]
        means = jnp.mean(cycles.reshape(shape), axis=axis + 1, keepdims=True)
        means = jnp.broadcast_to(means, shape).reshape(cycles.shape)
        result = jnp.where(width == size, means, result)
    return result


def reference(hydro_vars, face_b, widths, diffusion):
    fields = jnp.concatenate([hydro_vars, face_b], 0)
    theta_cells = fields.shape[3]
    polar_cycles = jnp.concatenate([fields[..., :CYCLES], fields[..., theta_cells - CYCLES:]], 3)
    averaged = block_means(polar_cycles, 2, widths)
    fields = jnp.concatenate([averaged[..., :CYCLES], fields[..., CYCLES:theta_cells - CYCLES], averaged[..., CYCLES:]], 3)
    hydro = fields[:5]
    change = fourth(hydro, 1, False) + fourth(hydro, 2, True) + fourth(hydro, 3, False)
    smoothed = hydro + diffusion[:, None, None, :] * change
    radial = fields[5]
    polar_face = fields[6]
    azimuth = fields[7]
    radial_next = jnp.concatenate([radial[1:], jnp.zeros_like(radial[:1])], 0)
    polar_next = jnp.concatenate([polar_face[..., 1:], jnp.zeros_like(polar_face[..., :1])], 2)
    azimuth_next = jnp.roll(azimuth, -1, axis=1)
    cell_field = 0.5 * jnp.stack([radial + radial_next, polar_face + polar_next, azimuth + azimuth_next])
    return jnp.concatenate([smoothed, cell_field], 0), fields[5:]
```

```python
import functools

import jax
import jax.numpy as jnp
from jax import lax
from jax.experimental import pallas as pl
from jax.experimental.pallas import tpu as pltpu
from jax.sharding import PartitionSpec as P

CYCLES = 8
HYDRO = 5
FIELDS = 8
LANES = 128
SLOTS = 2 * CYCLES
F32 = jnp.float32
ANY = pl.BlockSpec(memory_space=pl.ANY)
VMEM = pl.BlockSpec(memory_space=pltpu.VMEM)


def lane_index(shape):
    return lax.broadcasted_iota(jnp.int32, shape, len(shape) - 1)


def lane_widths(widths):
    slot = lane_index((1, LANES)) % SLOTS
    row = jnp.zeros((1, LANES), jnp.int32)
    for s in range(SLOTS):
        row = jnp.where(slot == s, widths[(s + CYCLES) % SLOTS], row)
    return row


def packed_shift(field):
    return (SLOTS * field + CYCLES) % LANES


def unpack(field, packed):
    return pltpu.roll(packed, (LANES - packed_shift(field)) % LANES, packed.ndim - 1)


def merge(field, spread, values, tile, tiles):
    lane = lane_index(values.shape)
    if tile == 0:
        values = jnp.where(lane < CYCLES, spread, values)
    if tile == tiles - 1:
        values = jnp.where(lane >= LANES - CYCLES, spread, values)
    return values


def lanes_of(tile):
    return slice(tile * LANES, (tile + 1) * LANES)


def with_polar(field, packed, values):
    tiles = values.shape[-1] // LANES
    spread = unpack(field, packed)
    parts = [merge(field, spread, values[..., lanes_of(t)], t, tiles) for t in range(tiles)]
    return jnp.concatenate(parts, values.ndim - 1)


def load_fields(h, b, buf, sems):
    copies = []
    for f in range(FIELDS):
        source = h.at[f] if f < HYDRO else b.at[f - HYDRO]
        copies.append([])
        for t in range(buf.shape[1]):
            copies[f].append(pltpu.make_async_copy(source.at[:, lanes_of(t)], buf.at[f, t], sems.at[f, t]))
    for field in copies:
        for copy in field:
            copy.start()
    return copies


def local_kernel(rows, cells, h, b, w, d, q, m, fw, bw, buf, pack, dv, wsm, sems, isems):
    tiles = buf.shape[1]
    size = rows * cells
    small = [pltpu.make_async_copy(w, wsm, sems.at[0]), pltpu.make_async_copy(d, dv, sems.at[1])]
    for copy in small:
        copy.start()
    copies = load_fields(h, b, buf, isems)
    small[0].wait()
    wl = lane_widths(wsm)
    lane = lane_index((size, LANES))
    for f in range(FIELDS):
        for copy in copies[f]:
            copy.wait()
        both = jnp.where(lane < CYCLES, buf[f, 0], buf[f, tiles - 1])
        spread = pltpu.roll(both, packed_shift(f), 1)
        pack[...] = spread if f == 0 else jnp.where(lane // SLOTS == f, spread, pack[...])
    cur = pack[...].reshape(size // 8, 8, LANES)
    result = cur
    place = lax.broadcasted_iota(jnp.int32, cur.shape, 1)
    span = 1
    while span < 8:
        other = jnp.where(place & span == 0, pltpu.roll(cur, 8 - span, 1), pltpu.roll(cur, span, 1))
        cur = cur + other
        span *= 2
        result = jnp.where(wl[None] == span, cur * (1.0 / span), result)
    cur = cur.reshape(rows, cells // 8, 8, LANES)
    while span < cells:
        group = span // 8
        parts = cur.reshape(rows, cells // (2 * span), 2, group, 8, LANES)
        both = parts[:, :, 0] + parts[:, :, 1]
        cur = jnp.stack([both, both], 2).reshape(cur.shape)
        span *= 2
        result = jnp.where(wl[None] == span, cur.reshape(result.shape) * (1.0 / span), result)
    spread = cur.reshape(result.shape) * (1.0 / cells)
    result = jnp.where(wl[None] >= cells, spread, result)
    q[...] = result.reshape(size, LANES)
    pack[...] = spread.reshape(size, LANES)
    m[...] = pack[pl.ds(0, rows, stride=cells), :]
    small[1].wait()

    def edge(f, cell):
        packed = jnp.where(wl >= 2 * cells, 0.0, q[pl.ds(cell, rows, stride=cells), :])
        spread = unpack(f, packed)
        return [merge(f, spread, buf[f, t, pl.ds(cell, rows, stride=cells), :], t, tiles) for t in range(tiles)]

    for f in range(HYDRO):
        for target, close, past in ((fw, cells - 1, cells - 2), (bw, 0, 1)):
            near, far = edge(f, close), edge(f, past)
            for t in range(tiles):
                scale = dv[f : f + 1, lanes_of(t)] * (1.0 / 12.0)
                target[2 * f, :, lanes_of(t)] = scale * (16.0 * near[t] - far[t])
                target[2 * f + 1, :, lanes_of(t)] = -scale * near[t]
    near = edge(FIELDS - 1, 0)
    for t in range(tiles):
        bw[2 * HYDRO, :, lanes_of(t)] = 0.5 * near[t]


def row_kernel(rows, cells, axis, h, b, w, d, g, q, mself, mout, up, dn, low, high, face, dv, wsm, sems):
    copies = [
        pltpu.make_async_copy(w, wsm, sems.at[0]),
        pltpu.make_async_copy(d, dv, sems.at[1]),
        pltpu.make_async_copy(h.at[:, pl.ds(0, 2 * cells), :], low, sems.at[2]),
        pltpu.make_async_copy(h.at[:, pl.ds((rows - 2) * cells, 2 * cells), :], high, sems.at[3]),
        pltpu.make_async_copy(b.at[0, pl.ds(0, cells), :], face, sems.at[4]),
    ]
    for copy in copies:
        copy.start()
    copies[0].wait()
    wl = lane_widths(wsm)
    pairs = g.shape[0]
    me = lax.axis_index(axis)
    mine = me // 2
    outer = jnp.where(me % 2 == 0, mine + pairs - 1, mine + 1) % pairs
    apart = mine ^ outer
    span, own, total_own, taken = 1, jnp.zeros(mself.shape, F32), jnp.zeros(mself.shape, F32), 0
    far = jnp.zeros(mself.shape, F32)
    while span <= pairs:
        for i in range(taken, span):
            total_own = total_own + g[i]
        taken = span
        start = (apart // span) * span
        total_far = g[start]
        for i in range(1, span):
            total_far = total_far + g[start + i]
        hit = wl == 2 * cells * span
        own = jnp.where(hit, total_own * (1.0 / span), own)
        far = jnp.where(hit, total_far * (1.0 / span), far)
        span *= 2
    mself[...] = own
    mout[...] = far
    for copy in copies[1:]:
        copy.wait()

    def polar_row(r):
        local = q[r * cells : (r + 1) * cells, :]
        return jnp.where(wl >= 2 * cells, jnp.broadcast_to(own[r : r + 1, :], local.shape), local)

    top, below = polar_row(rows - 1), polar_row(rows - 2)
    first, second = polar_row(0), polar_row(1)
    for f in range(HYDRO):
        scale = dv[f : f + 1, :] * (1.0 / 12.0)
        near, past = with_polar(f, top, high[f, cells:, :]), with_polar(f, below, high[f, :cells, :])
        up[2 * f] = scale * (16.0 * near - past)
        up[2 * f + 1] = -scale * near
        near, past = with_polar(f, first, low[f, :cells, :]), with_polar(f, second, low[f, cells:, :])
        dn[2 * f] = scale * (16.0 * near - past)
        dn[2 * f + 1] = -scale * near
    dn[2 * HYDRO] = 0.5 * with_polar(HYDRO, first, face[...])


def lane_shift(parts, by):
    lane = lane_index(parts[0].shape)
    rolled = [pltpu.roll(part, by % LANES, 1) for part in parts]
    zero = jnp.zeros_like(parts[0])
    if by > 0:
        return [jnp.where(lane < by, rolled[t - 1] if t > 0 else zero, rolled[t]) for t in range(len(parts))]
    after = rolled[1:] + [zero]
    return [jnp.where(lane >= LANES + by, after[t], rolled[t]) for t in range(len(parts))]


def cell_shift(part, by):
    cells = part.shape[0]
    place = lax.broadcasted_iota(jnp.int32, part.shape, 0)
    inside = place >= by if by > 0 else place < cells + by
    return jnp.where(inside, pltpu.roll(part, by % cells, 0), 0.0)


def main_kernel(rows, cells, axis, h, b, w, d, q, mself, mout, up, dn, cons, faces, e, buf, pad, pol, cell, dv, wsm, sems, isems, osems):
    tiles = buf.shape[1]
    size = rows * cells
    small = [pltpu.make_async_copy(w, wsm, sems.at[0]), pltpu.make_async_copy(d, dv, sems.at[1])]
    for copy in small:
        copy.start()
    copies = load_fields(h, b, buf, isems)
    for copy in small:
        copy.wait()
    wl = lane_widths(wsm)
    wide = wl >= 2 * cells
    spread = jnp.broadcast_to(mself[...][:, None, :], (rows, cells, LANES)).reshape(size, LANES)
    pol[...] = jnp.where(wide, spread, q[...])
    even = lax.axis_index(axis) % 2 == 0
    left = jnp.where(wide, jnp.where(even, mout[...], mself[...]), 0.0)
    right = jnp.where(wide, jnp.where(even, mself[...], mout[...]), 0.0)
    pad[:, 0 : 2 * cells, :] = jnp.zeros((tiles, 2 * cells, LANES), F32)
    pad[:, 2 * cells + size :, :] = jnp.zeros((tiles, 2 * cells, LANES), F32)
    outs = []

    def put(source, target, sem):
        for t in range(tiles):
            outs.append(pltpu.make_async_copy(source.at[t], target.at[:, lanes_of(t)], sem.at[t]))
            outs[-1].start()

    def edge(f, cell_of, ref):
        return [ref[f, t, pl.ds(cell_of, rows, stride=cells), :] for t in range(tiles)]

    def polar_part(f, packed):
        spread = unpack(f, packed)
        return [merge(f, spread, jnp.zeros(spread.shape, F32), t, tiles) for t in range(tiles)]

    for f in range(HYDRO):
        for copy in copies[f]:
            copy.wait()
        spread = unpack(f, pol[...])
        for t in range(tiles):
            pad[t, 2 * cells : 2 * cells + size, :] = merge(f, spread, buf[f, t], t, tiles)
        scales = [dv[f : f + 1, lanes_of(t)] * (1.0 / 12.0) for t in range(tiles)]

        def step(r, carry):
            base = pl.multiple_of(r * cells, cells)
            v = [pad[t, pl.ds(base + 2 * cells, cells), :] for t in range(tiles)]
            before, after = lane_shift(v, 1), lane_shift(v, -1)
            before2, after2 = lane_shift(v, 2), lane_shift(v, -2)
            for t in range(tiles):
                one = pad[t, pl.ds(base + cells, cells), :] + pad[t, pl.ds(base + 3 * cells, cells), :]
                two = pad[t, pl.ds(base, cells), :] + pad[t, pl.ds(base + 4 * cells, cells), :]
                one = one + before[t] + after[t] + cell_shift(v[t], 1) + cell_shift(v[t], -1)
                two = two + before2[t] + after2[t] + cell_shift(v[t], 2) + cell_shift(v[t], -2)
                buf[f, t, pl.ds(base, cells), :] = v[t] + scales[t] * (16.0 * one - two - 90.0 * v[t])
            return carry

        lax.fori_loop(0, rows, step, 0, unroll=2)
        near, far = polar_part(f, left), polar_part(f, right)
        for t in range(tiles):
            buf[f, t, 0:cells, :] += up[2 * f, :, lanes_of(t)]
            buf[f, t, cells : 2 * cells, :] += up[2 * f + 1, :, lanes_of(t)]
            buf[f, t, size - cells :, :] += dn[2 * f, :, lanes_of(t)]
            buf[f, t, size - 2 * cells : size - cells, :] += dn[2 * f + 1, :, lanes_of(t)]
        for j, (cell_of, polar, factor) in enumerate(((0, near, 15.0), (1, near, -1.0), (cells - 1, far, 15.0), (cells - 2, far, -1.0))):
            own = edge(f, cell_of, buf)
            for t in range(tiles):
                e[4 * f + j, :, lanes_of(t)] = own[t] + (factor * scales[t]) * polar[t]
        put(buf.at[f], cons.at[f], osems.at[f])
    for k in range(FIELDS - HYDRO):
        f = HYDRO + k
        for copy in copies[f]:
            copy.wait()
        spread = unpack(f, pol[...])
        for t in range(tiles):
            buf[f, t] = merge(f, spread, buf[f, t], t, tiles)
        put(buf.at[f], faces.at[k], osems.at[FIELDS + k])
        if k == 0:
            for t in range(tiles):
                cell[k, t, : size - cells, :] = 0.5 * (buf[f, t, : size - cells, :] + buf[f, t, cells:, :])
                cell[k, t, size - cells :, :] = 0.5 * buf[f, t, size - cells :, :] + dn[2 * HYDRO, :, lanes_of(t)]
        else:

            def step(r, carry):
                base = pl.multiple_of(r * cells, cells)
                v = [buf[f, t, pl.ds(base, cells), :] for t in range(tiles)]
                after = lane_shift(v, -1) if k == 1 else [cell_shift(part, -1) for part in v]
                for t in range(tiles):
                    cell[k, t, pl.ds(base, cells), :] = 0.5 * (v[t] + after[t])
                return carry

            lax.fori_loop(0, rows, step, 0, unroll=2)
        if k == 2:
            own, far = edge(k, cells - 1, cell), polar_part(f, right)
            for t in range(tiles):
                e[4 * HYDRO, :, lanes_of(t)] = own[t] + 0.5 * far[t]
        put(cell.at[k], cons.at[f], osems.at[f])
    for copy in outs:
        copy.wait()


def edge_kernel(rows, cells, cons_in, e, fw, bw, cons, done, sems):
    del cons_in
    copies = []
    places = (0, 1, cells - 1, cells - 2)
    for f in range(HYDRO):
        for j in range(2):
            done[4 * f + j] = e[4 * f + j] + fw[2 * f + j]
            done[4 * f + 2 + j] = e[4 * f + 2 + j] + bw[2 * f + j]
        for j in range(4):
            copies.append(pltpu.make_async_copy(done.at[4 * f + j], cons.at[f, :, places[j], :], sems.at[4 * f + j]))
            copies[-1].start()
    done[4 * HYDRO] = e[4 * HYDRO] + bw[2 * HYDRO]
    copies.append(pltpu.make_async_copy(done.at[4 * HYDRO], cons.at[FIELDS - 1, :, cells - 1, :], sems.at[4 * HYDRO]))
    copies[-1].start()
    for copy in copies:
        copy.wait()


def params(mib):
    return pltpu.CompilerParams(vmem_limit_bytes=mib * 1024 * 1024)


def cost(flops, size):
    return pl.CostEstimate(flops=flops, bytes_accessed=size, transcendentals=0)


def body(hydro_vars, face_b, widths, diffusion):
    _, rows, cells, total = hydro_vars.shape
    size = rows * cells
    tiles = total // LANES
    count = lax.axis_size("phi")
    layers = lax.axis_size("row")
    h = hydro_vars.reshape(HYDRO, size, total)
    b = face_b.reshape(FIELDS - HYDRO, size, total)
    dma = pltpu.SemaphoreType.DMA

    def shape(*dims):
        return jax.ShapeDtypeStruct(dims, F32)

    q, m, fw, bw = pl.pallas_call(
        functools.partial(local_kernel, rows, cells),
        out_shape=[shape(size, LANES), shape(rows, LANES), shape(2 * HYDRO, rows, total), shape(2 * HYDRO + 1, rows, total)],
        in_specs=[ANY] * 4,
        out_specs=[VMEM] * 4,
        scratch_shapes=[
            pltpu.VMEM((FIELDS, tiles, size, LANES), F32),
            pltpu.VMEM((size, LANES), F32),
            pltpu.VMEM((HYDRO, total), F32),
            pltpu.SMEM((SLOTS,), jnp.int32),
            dma((2,)),
            dma((FIELDS, tiles)),
        ],
        compiler_params=params(12),
        cost_estimate=cost(5_000_000, 5_000_000),
        name="local",
    )(h, b, widths, diffusion)

    pair = lax.ppermute(m, "phi", [(i, i ^ 1) for i in range(count)])
    fw = lax.ppermute(fw, "phi", [(i, (i + 1) % count) for i in range(count)])
    bw = lax.ppermute(bw, "phi", [((i + 1) % count, i) for i in range(count)])
    g = (0.5 * (m + pair))[None]
    step = 2
    while step < count:
        g = jnp.concatenate([g, lax.ppermute(g, "phi", [(i, i ^ step) for i in range(count)])], 0)
        step *= 2

    mself, mout, up, dn = pl.pallas_call(
        functools.partial(row_kernel, rows, cells, "phi"),
        out_shape=[shape(rows, LANES), shape(rows, LANES), shape(2 * HYDRO, cells, total), shape(2 * HYDRO + 1, cells, total)],
        in_specs=[ANY] * 4 + [VMEM] * 2,
        out_specs=[VMEM] * 4,
        scratch_shapes=[
            pltpu.VMEM((HYDRO, 2 * cells, total), F32),
            pltpu.VMEM((HYDRO, 2 * cells, total), F32),
            pltpu.VMEM((cells, total), F32),
            pltpu.VMEM((HYDRO, total), F32),
            pltpu.SMEM((SLOTS,), jnp.int32),
            dma((5,)),
        ],
        compiler_params=params(8),
        cost_estimate=cost(2_000_000, 1_000_000),
        name="rows",
    )(h, b, widths, diffusion, g, q)
    up = lax.ppermute(up, "row", [(i, i + 1) for i in range(layers - 1)])
    dn = lax.ppermute(dn, "row", [(i + 1, i) for i in range(layers - 1)])

    cons, faces, e = pl.pallas_call(
        functools.partial(main_kernel, rows, cells, "phi"),
        out_shape=[shape(FIELDS, size, total), shape(FIELDS - HYDRO, size, total), shape(4 * HYDRO + 1, rows, total)],
        in_specs=[ANY] * 4 + [VMEM] * 5,
        out_specs=[ANY, ANY, VMEM],
        scratch_shapes=[
            pltpu.VMEM((FIELDS, tiles, size, LANES), F32),
            pltpu.VMEM((tiles, size + 4 * cells, LANES), F32),
            pltpu.VMEM((size, LANES), F32),
            pltpu.VMEM((FIELDS - HYDRO, tiles, size, LANES), F32),
            pltpu.VMEM((HYDRO, total), F32),
            pltpu.SMEM((SLOTS,), jnp.int32),
            dma((2,)),
            dma((FIELDS, tiles)),
            dma((2 * FIELDS - HYDRO, tiles)),
        ],
        compiler_params=params(16),
        cost_estimate=cost(20_000_000, 10_000_000),
        name="main",
    )(h, b, widths, diffusion, q, mself, mout, up, dn)

    cons = pl.pallas_call(
        functools.partial(edge_kernel, rows, cells),
        out_shape=shape(FIELDS, rows, cells, total),
        in_specs=[ANY] + [VMEM] * 3,
        out_specs=ANY,
        scratch_shapes=[pltpu.VMEM((4 * HYDRO + 1, rows, total), F32), dma((4 * HYDRO + 1,))],
        input_output_aliases={0: 0},
        compiler_params=params(8),
        cost_estimate=cost(1_000_000, 1_000_000),
        name="edges",
    )(cons.reshape(FIELDS, rows, cells, total), e, fw, bw)
    return cons, faces.reshape(FIELDS - HYDRO, rows, cells, total)


def solution(mesh):
    in_specs = (P(None, "row", "phi", None), P(None, "row", "phi", None), P(), P())
    out_specs = (P(None, "row", "phi", None), P(None, "row", "phi", None))
    return jax.shard_map(body, mesh=mesh, in_specs=in_specs, out_specs=out_specs, check_vma=False)
```
